32 devices in a mesh: dp: 8 (over z, x), expert: 4 (over y, core).
Axes of the slice: x: 2, y: 2, z: 4, core: 2. Of those that a mesh axis runs over, the one named last changes fastest.
Arguments:
- tokens: bfloat16 [4096, 4096], P(('dp', 'expert')), may hold values from -6 to 6
- grad_out: bfloat16 [4096, 4096], P(('dp', 'expert')), may hold values from -6 to 6
- experts: int32 [4096, 2], P(('dp', 'expert')), may hold values from 0 to 7, all different within a row; in each aligned block of 128 rows (0 to 127, 128 to 255, ...) at most 64 rows name the same one
- gates: bfloat16 [4096, 2], P(('dp', 'expert')), may hold values from 0 to 1, as said below
- router_weight: bfloat16 [8, 4096], replicated, may hold values from -3 to 3
- saved_outputs: bfloat16 [16384, 4096], P(('dp', 'expert')), may hold values from -0.19921875 to 0.19921875
Outputs:
- input_grad: bfloat16 [4096, 4096], P(('dp', 'expert'))
- router_grad: float32 [8, 4096], replicated
- expert_grad: bfloat16 [16384, 4096], P(('dp', 'expert'))
The draws below stay inside these ranges and needn't reach their ends.
Inputs may be any that keep to these rules, and one draw needn't show every extreme that they name: Within each aligned block of 128 tokens (the tokens of one device), no expert is named by more than 64 slots, and in some blocks an expert is named by exactly 64 slots. The two experts of a token differ. The two gates of a token are positive and add up to one, up to rounding to bfloat16.
All inputs are finite; a program needn't handle non-finite values.
Results may differ from the reference program's by a relative error of at most 0.0085.
Values may be sent and summed in bfloat16 or wider, within the bound.
A program may use at most 64 MiB of HBM per device.

```python
import math
import jax
import jax.numpy as jnp
import numpy as np
from jax import lax

D = 4096
TOPK = 2
TOK_DEV = 128
EXPERTS = 8
MOST = 64
TOKENS = 4096
SLOTS = 16384
N_DP = 8
N_EXPERT = 4


def draw_gates(key, part):
    leading = jax.random.uniform(key, (TOKENS, 1), jnp.float32, 0.1, 0.9)
    return jnp.concatenate([leading, 1.0 - leading], axis=1).astype(jnp.bfloat16)


def shard_levels(key, dims, split, low, high):
    gain, own = 1.0, jax.random.fold_in(key, 6)
    for dim, shards_of in split:
        steps = jnp.exp(jax.random.uniform(jax.random.fold_in(own, dim), (shards_of,), jnp.float32, low / len(split), high / len(split)))
        gain = gain * jnp.repeat(steps, dims[dim] // shards_of).reshape([-1 if axis == dim else 1 for axis in range(len(dims))])
    return gain


def assign_block(key, own, number, rows, amount, top, bound, lean):
    ranking = jax.random.permutation(key, amount)
    crowded, common = load_shares(amount, rows * top, bound, lean, True), load_shares(amount, rows * top, bound, lean, False)
    places = jnp.arange(amount)

    def named(sizes, rotation):
        used = int((sizes > 0).sum())
        fixed = max(1, used // 4)
        shifted = fixed + (places - fixed + rotation * (used - fixed)) % max(1, amount - fixed)
        return jnp.zeros((amount,), jnp.int32).at[ranking[jnp.where(places < fixed, places, shifted)]].set(jnp.asarray(sizes, jnp.int32))

    sizes = jnp.where(number % 4 == 0, named(crowded, number // 4), named(common, number - number // 4 - 1))
    mixed = jax.random.permutation(jax.random.fold_in(own, 3), amount)
    donor, receiver = mixed[0:amount // 2 * 2:2], mixed[1:amount // 2 * 2:2]
    room = jnp.minimum(sizes[donor] - 1, bound - sizes[receiver]) // 2
    room = jnp.where((donor == ranking[0]) | (receiver == ranking[0]) | (sizes[receiver] == 0), 0, jnp.maximum(room, 0))
    shifted = jax.random.randint(jax.random.fold_in(own, 4), (amount // 2,), 0, 1 << 20) % (room + 1)
    sizes = sizes.at[donor].add(-shifted).at[receiver].add(shifted)
    labels = jnp.searchsorted(jnp.cumsum(sizes), jnp.arange(rows * top), side="right").astype(jnp.int32)
    grid = labels.reshape(top, rows).T
    grid = grid[jax.random.permutation(jax.random.fold_in(own, 1), rows)]
    rotation = jax.random.randint(jax.random.fold_in(own, 2), (rows, 1), 0, top)
    return jnp.take_along_axis(grid, (jnp.arange(top)[None, :] + rotation) % top, axis=1)


def load_shares(number_of, total, bound, lean, full):
    weights = [(1 << 20) // math.isqrt(standing ** lean) + 1 for standing in range(1, number_of + 1)]
    largest = bound if full else min(bound, max(-(-total // number_of), total * weights[0] // sum(weights)))
    least = 1 if total - largest >= number_of - 1 else 0
    given, rest = [largest] + [least] * (number_of - 1), total - largest - least * (number_of - 1)
    while rest > 0:
        candidates = [i for i in range(1, number_of) if given[i] < largest] or [i for i in range(1, number_of) if given[i] < bound]
        pool, budget = sum([weights[i] for i in candidates]), rest
        for i in candidates:
            extra = min(bound - given[i], max(1, budget * weights[i] // pool), rest)
            given[i] = given[i] + extra
            rest = rest - extra
    return np.array(given)


def bell_draw(key, dims, deviation, bound, pieces=(), kind=jnp.bfloat16):
    values = jax.random.normal(key, dims, jnp.float32) * deviation
    if len(pieces) > 0:
        values = shard_levels(key, dims, pieces, -0.22, 0.18) * values
    return jnp.clip(values, min=-bound, max=bound).astype(kind)


def setup_inputs(seed: int = 0) -> dict:
    seeds = jax.random.split(jax.random.key(seed), 7)
    tokens = bell_draw(seeds[0], (TOKENS, D), 1.0, 6.0, ((0, 32),))
    grad_out = bell_draw(seeds[1], (TOKENS, D), 1.0, 6.0, ((0, 32),))
    experts_keys = jax.random.split(jax.random.fold_in(seeds[2], 1), TOKENS // TOK_DEV)
    experts_turns = jax.random.permutation(jax.random.fold_in(seeds[2], 3), TOKENS // TOK_DEV)
    experts = jax.vmap(lambda own, number: assign_block(jax.random.fold_in(seeds[2], 2), own, number, TOK_DEV, EXPERTS, TOPK, MOST, 2))(experts_keys, experts_turns).reshape((TOKENS, TOPK))
    gates = draw_gates(jax.random.fold_in(seeds[6], 71), 0)
    router_weight = bell_draw(seeds[4], (EXPERTS, D), 0.5, 3.0)
    saved_outputs = bell_draw(seeds[5], (SLOTS, D), 0.03125, 0.19921875, ((0, 32),))
    return {"tokens": tokens, "grad_out": grad_out, "experts": experts, "gates": gates, "router_weight": router_weight, "saved_outputs": saved_outputs}


def slot_positions(chosen):
    slot_expert = chosen.reshape(-1).astype(jnp.int32)
    onehot = (slot_expert[:, None] == jnp.arange(EXPERTS, dtype=jnp.int32)[None, :]).astype(jnp.int32)
    before = jnp.cumsum(onehot, axis=0) - onehot
    position = jnp.sum(before * onehot, axis=1).astype(jnp.int32)
    return slot_expert, position


def reference(tokens, grad_out, experts, gates, router_weight, saved_outputs):
    groups = N_EXPERT
    shaped = (
        tokens.reshape(N_DP, groups, TOK_DEV, D),
        grad_out.reshape(N_DP, groups, TOK_DEV, D),
        experts.reshape(N_DP, groups, TOK_DEV, TOPK),
        gates.reshape(N_DP, groups, TOK_DEV, TOPK),
        saved_outputs.reshape(N_DP, EXPERTS, groups, MOST, D),
    )

    def one_shard(inputs):
        feature, upstream, chosen, gate_raw, stored = inputs
        slot_expert, position = jax.vmap(slot_positions)(chosen)
        source = jnp.broadcast_to(jnp.arange(groups, dtype=jnp.int32)[:, None], slot_expert.shape)
        picked = stored[slot_expert, source, position]
        repeated = jnp.repeat(upstream, TOPK, axis=1)
        products = jnp.sum(repeated.astype(jnp.float32) * picked.astype(jnp.float32), axis=-1)
        gate_grad = products.reshape(groups, TOK_DEV, TOPK)
        gate_values = gate_raw.astype(jnp.float32)
        blended = jnp.sum(gate_values * gate_grad, axis=-1, keepdims=True)
        slot_grad = gate_values * (gate_grad - blended)
        onehot = (chosen[..., None] == jnp.arange(EXPERTS, dtype=jnp.int32)).astype(jnp.float32)
        logit_grad = jnp.sum(onehot * slot_grad[..., None], axis=2).astype(jnp.bfloat16)
        partial_value = jnp.einsum("ste,std->ed", logit_grad.astype(jnp.float32), feature.astype(jnp.float32))
        through = jnp.einsum("ste,ed->std", logit_grad.astype(jnp.float32), router_weight.astype(jnp.float32))
        weighted = (gate_values.reshape(groups, TOK_DEV * TOPK)[..., None] * repeated.astype(jnp.float32)).astype(jnp.bfloat16)
        scattered = jnp.zeros((EXPERTS, groups, MOST, D), jnp.bfloat16).at[slot_expert, source, position].set(weighted)
        return partial_value, through.astype(jnp.bfloat16), scattered

    partials, through, scattered = lax.map(one_shard, shaped)
    router_grad = jnp.sum(partials, axis=0) * (TOKENS ** -0.5)
    return through.reshape(TOKENS, D), router_grad, scattered.reshape(SLOTS, D)
```

```python
import functools

import jax
import jax.numpy as jnp
from jax import lax
from jax.experimental import pallas as pl
from jax.experimental.pallas import tpu as pltpu
from jax.sharding import PartitionSpec as P

MESH = pl.DeviceIdType.MESH
F32 = jnp.float32
BF16 = jnp.bfloat16


def exchange_kernel(
    n, m, pieces, scale,
    info_ref, g_ref, tok_ref, saved_ref,
    g_out, w_out, logit_out, router_out,
    slots, saved_v, tok_v, meta_own, meta_in, ret_own, ret_in,
    acc_a, acc_b, part, part_in, dp_in, fin, fin_in,
    g_send, g_recv, meta_send, meta_recv, ret_send, ret_recv,
    part_send, part_recv, dp_send, dp_recv, fin_send, fin_recv,
    saved_sem, tok_sem, gout_sem,
):
    held, _, cap, width = saved_ref.shape
    rows = held * cap
    tokens = g_ref.shape[0]
    experts = logit_out.shape[1]
    piece = width // pieces
    share = width // n
    pairs = n // 2
    me = lax.axis_index("expert")
    dp = lax.axis_index("dp")
    parity = me % 2
    pair = me // 2

    def source(j):
        q, flip = j // 2, j % 2
        low = parity if flip == 0 else 1 - parity
        return ((pair - q + pairs) % pairs) * 2 + low

    def target(j):
        q, flip = j // 2, j % 2
        low = parity if flip == 0 else 1 - parity
        return ((pair + q) % pairs) * 2 + low

    def cols(c):
        return pl.ds(pl.multiple_of(c * piece, piece), piece)

    barrier = pltpu.get_barrier_semaphore()
    for j in range(1, n):
        pl.semaphore_signal(barrier, inc=1, device_id={"expert": target(j)}, device_id_type=MESH)

    def greet(i, carry):
        pl.semaphore_signal(barrier, inc=1, device_id={"dp": (dp + i) % m}, device_id_type=MESH)
        return carry

    lax.fori_loop(1, m, greet, 0)

    def saved_copy(j, h):
        return pltpu.make_async_copy(
            saved_ref.at[h, source(j)],
            saved_v.at[j, pl.ds(h * cap, cap)],
            saved_sem.at[j, h],
        )

    for j in range(n):
        for h in range(held):
            saved_copy(j, h).start()
    tok_copy = pltpu.make_async_copy(tok_ref, tok_v, tok_sem)
    tok_copy.start()
    own_out = pltpu.make_async_copy(g_ref, g_out.at[me], gout_sem.at[0])
    own_out.start()

    expert_ids = lax.broadcasted_iota(jnp.int32, (experts, tokens), 0).astype(F32)
    hot = [(info_ref[k : k + 1, :] == expert_ids).astype(F32) for k in range(2)]
    earlier = (
        lax.broadcasted_iota(jnp.int32, (tokens, tokens), 0)
        < lax.broadcasted_iota(jnp.int32, (tokens, tokens), 1)
    ).astype(F32).astype(BF16)
    before = jnp.dot((hot[0] + hot[1]).astype(BF16), earlier, preferred_element_type=F32)
    meta_own[...] = info_ref[...]
    for k in range(2):
        position = jnp.sum(before * hot[k], axis=0, keepdims=True)
        meta_own[k : k + 1, :] = info_ref[k : k + 1, :] * float(cap) + position

    pl.semaphore_wait(barrier, n + m - 2)

    def g_copy(src, j, c, to):
        return pltpu.make_async_remote_copy(
            src_ref=src,
            dst_ref=slots.at[j - 1, :, cols(c)],
            send_sem=g_send.at[j - 1, c],
            recv_sem=g_recv.at[j - 1, c],
            device_id={"expert": to},
            device_id_type=MESH,
        )

    def small_copy(src, dst, send, recv, j, to):
        return pltpu.make_async_remote_copy(
            src_ref=src,
            dst_ref=dst.at[j - 1],
            send_sem=send.at[j - 1],
            recv_sem=recv.at[j - 1],
            device_id={"expert": to},
            device_id_type=MESH,
        )

    meta_copies = [
        small_copy(meta_own, meta_in, meta_send, meta_recv, j, target(j)) for j in range(1, n)
    ]
    for copy in meta_copies:
        copy.start()
    for q in range(1, pairs):

        def send_direct(c, carry, q=q):
            g_copy(g_ref.at[:, cols(c)], 2 * q, c, target(2 * q)).start()
            return carry

        lax.fori_loop(0, pieces, send_direct, 0)

    def send_partner(c, carry):
        g_copy(g_ref.at[:, cols(c)], 1, c, target(1)).start()
        return carry

    lax.fori_loop(0, pieces, send_partner, 0)

    row_ids = lax.broadcasted_iota(jnp.int32, (rows, tokens), 0).astype(F32)
    base = (me * rows).astype(F32)

    def masks(meta):
        return [meta[k : k + 1, :] - base == row_ids for k in range(2)]

    def write_weights(j, meta):
        named = masks(meta)
        weights = jnp.where(named[0], meta[2:3, :], 0.0) + jnp.where(named[1], meta[3:4, :], 0.0)
        w_out[source(j)] = weights.astype(BF16)

    def product(j, c, right):
        return lax.dot_general(
            saved_v[j, :, cols(c)], right, (((1,), (1,)), ((), ())), preferred_element_type=F32
        )

    def picked(meta, total):
        return [
            jnp.sum(jnp.where(named, total, 0.0), axis=0, keepdims=True) for named in masks(meta)
        ]

    def wait_saved(j):
        for h in range(held):
            saved_copy(j, h).wait()

    ret_copies = [
        small_copy(ret_own.at[j - 1], ret_in, ret_send, ret_recv, j, source(j))
        for j in range(1, n)
    ]

    def give_back(j, total):
        first, second = picked(meta_in[j - 1], total)
        ret_own[j - 1, 0:1, :] = first
        ret_own[j - 1, 1:2, :] = second
        ret_copies[j - 1].start()

    ret_own[...] = jnp.zeros_like(ret_own)
    wait_saved(0)
    write_weights(0, meta_own[...])
    zero = jnp.zeros((rows, tokens), F32)
    own_total = lax.fori_loop(
        0, pieces, lambda c, total: total + product(0, c, g_ref[:, cols(c)]), zero
    )
    own_first, own_second = picked(meta_own[...], own_total)

    for j in range(1, n):
        meta_copies[j - 1].wait_recv()
        write_weights(j, meta_in[j - 1])

    def arrived(j, c):
        g_copy(slots.at[j - 1, :, cols(c)], j, c, target(j)).wait_recv()

    def take(j, c, acc):
        acc[...] += product(j, c, slots[j - 1, :, cols(c)])

    outs = [own_out]

    def put_out(j):
        copy = pltpu.make_async_copy(slots.at[j - 1], g_out.at[source(j)], gout_sem.at[j])
        copy.start()
        outs.append(copy)

    acc_a[...] = zero
    wait_saved(1)

    def partner_step(c, carry):
        arrived(1, c)
        take(1, c, acc_a)
        return carry

    lax.fori_loop(0, pieces, partner_step, 0)
    put_out(1)
    give_back(1, acc_a[...])

    for q in range(1, pairs):
        direct, relayed = 2 * q, 2 * q + 1
        acc_a[...] = zero
        acc_b[...] = zero
        wait_saved(direct)
        wait_saved(relayed)

        def direct_step(c, direct=direct, relayed=relayed):
            arrived(direct, c)
            g_copy(slots.at[direct - 1, :, cols(c)], relayed, c, target(1)).start()
            take(direct, c, acc_a)

        def relayed_step(c, relayed=relayed):
            arrived(relayed, c)
            take(relayed, c, acc_b)

        direct_step(0)

        def step(c, carry, direct_step=direct_step, relayed_step=relayed_step):
            direct_step(c)
            relayed_step(c - 1)
            return carry

        lax.fori_loop(1, pieces, step, 0)
        put_out(direct)
        give_back(direct, acc_a[...])
        relayed_step(pieces - 1)
        put_out(relayed)
        give_back(relayed, acc_b[...])

    grads = [own_first, own_second]
    for j in range(1, n):
        ret_copies[j - 1].wait_recv()
        grads = [grads[k] + ret_in[j - 1, k : k + 1, :] for k in range(2)]
    gates = [info_ref[2 + k : 3 + k, :] for k in range(2)]
    blended = gates[0] * grads[0] + gates[1] * grads[1]
    logit = hot[0] * (gates[0] * (grads[0] - blended)) + hot[1] * (gates[1] * (grads[1] - blended))
    logit_low = logit.astype(BF16)
    tok_copy.wait()
    for j in range(n):
        part[j] = jnp.dot(
            logit_low, tok_v[:, j * share : (j + 1) * share], preferred_element_type=F32
        )

    part_copies = [
        small_copy(part.at[target(j)], part_in, part_send, part_recv, j, target(j))
        for j in range(1, n)
    ]
    for copy in part_copies:
        copy.start()
    logit_out[...] = logit.T.astype(BF16)
    total = part[me]
    for j in range(1, n):
        part_copies[j - 1].wait_recv()
        total = total + part_in[j - 1]
    dp_in[dp] = total

    def dp_copy(slot, i):
        return pltpu.make_async_remote_copy(
            src_ref=dp_in.at[dp],
            dst_ref=dp_in.at[slot],
            send_sem=dp_send.at[i],
            recv_sem=dp_recv.at[i],
            device_id={"dp": (dp + i) % m},
            device_id_type=MESH,
        )

    def dp_start(i, carry):
        dp_copy(dp, i).start()
        return carry

    def dp_wait(i, carry):
        dp_copy((dp - i + m) % m, i).wait_recv()
        return carry

    lax.fori_loop(1, m, dp_start, 0)
    lax.fori_loop(1, m, dp_wait, 0)
    fin[...] = (
        lax.fori_loop(0, m, lambda i, t: t + dp_in[i], jnp.zeros((experts, share), F32)) * scale
    )
    fin_copies = [small_copy(fin, fin_in, fin_send, fin_recv, j, target(j)) for j in range(1, n)]
    for copy in fin_copies:
        copy.start()

    def lanes(k):
        return pl.ds(pl.multiple_of(k * share, share), share)

    router_out[:, lanes(me)] = fin[...]

    def g_sent(c, carry):
        g_copy(g_ref.at[:, cols(c)], 1, c, target(1)).wait_send()
        for q in range(1, pairs):
            g_copy(g_ref.at[:, cols(c)], 2 * q, c, target(2 * q)).wait_send()
            g_copy(slots.at[2 * q - 1, :, cols(c)], 2 * q + 1, c, target(1)).wait_send()
        return carry

    lax.fori_loop(0, pieces, g_sent, 0)

    def dp_sent(i, carry):
        dp_copy(dp, i).wait_send()
        return carry

    lax.fori_loop(1, m, dp_sent, 0)
    for copy in meta_copies + ret_copies + part_copies + fin_copies:
        copy.wait_send()
    for copy in outs:
        copy.wait()
    for j in range(1, n):
        fin_copies[j - 1].wait_recv()
        router_out[:, lanes(source(j))] = fin_in[j - 1]


def exchange(info, grad_out, tokens, saved, experts, n, m):
    held, _, cap, width = saved.shape
    count = tokens.shape[0]
    rows = held * cap
    pieces = max(1, width // 512)
    share = width // n
    scale = float(m * n * count) ** (-0.5)
    dma = pltpu.SemaphoreType.DMA
    vmem = pl.BlockSpec(memory_space=pltpu.VMEM)
    anywhere = pl.BlockSpec(memory_space=pl.ANY)
    return pl.pallas_call(
        functools.partial(exchange_kernel, n, m, pieces, scale),
        name="exchange",
        out_shape=(
            jax.ShapeDtypeStruct((n, count, width), BF16),
            jax.ShapeDtypeStruct((n, rows, count), BF16),
            jax.ShapeDtypeStruct((count, experts), BF16),
            jax.ShapeDtypeStruct((experts, width), F32),
        ),
        in_specs=[vmem, vmem, anywhere, anywhere],
        out_specs=(anywhere, vmem, vmem, vmem),
        scratch_shapes=[
            pltpu.VMEM((n - 1, count, width), BF16),
            pltpu.VMEM((n, rows, width), BF16),
            pltpu.VMEM((count, width), BF16),
            pltpu.VMEM((8, count), F32),
            pltpu.VMEM((n - 1, 8, count), F32),
            pltpu.VMEM((n - 1, 8, count), F32),
            pltpu.VMEM((n - 1, 8, count), F32),
            pltpu.VMEM((rows, count), F32),
            pltpu.VMEM((rows, count), F32),
            pltpu.VMEM((n, experts, share), F32),
            pltpu.VMEM((n - 1, experts, share), F32),
            pltpu.VMEM((m, experts, share), F32),
            pltpu.VMEM((experts, share), F32),
            pltpu.VMEM((n - 1, experts, share), F32),
            dma((n - 1, pieces)), dma((n - 1, pieces)),
            dma((n - 1,)), dma((n - 1,)),
            dma((n - 1,)), dma((n - 1,)),
            dma((n - 1,)), dma((n - 1,)),
            dma((m,)), dma((m,)),
            dma((n - 1,)), dma((n - 1,)),
            dma((n, held)), dma, dma((n,)),
        ],
        compiler_params=pltpu.CompilerParams(
            collective_id=0, has_side_effects=True, vmem_limit_bytes=48 << 20
        ),
    )(info, grad_out, tokens, saved)


def finish_kernel(w_ref, g_ref, logit_ref, rw_ref, eg_ref, ig_ref):
    held, cap = eg_ref.shape[0], eg_ref.shape[2]
    spread = jnp.dot(w_ref[0], g_ref[0], preferred_element_type=F32).astype(BF16)
    for h in range(held):
        eg_ref[h, 0] = spread[h * cap : (h + 1) * cap]
    ig_ref[...] = jnp.dot(logit_ref[...], rw_ref[...], preferred_element_type=F32).astype(BF16)


def finish(weights, gathered, logit, router_weight, layout):
    held, n, cap, width = layout
    count, experts = logit.shape
    rows = held * cap
    split = 2
    block = width // split
    return pl.pallas_call(
        finish_kernel,
        name="finish",
        grid=(n, split),
        out_shape=(
            jax.ShapeDtypeStruct(layout, BF16),
            jax.ShapeDtypeStruct((count, width), BF16),
        ),
        in_specs=[
            pl.BlockSpec((1, rows, count), lambda s, c: (s, 0, 0)),
            pl.BlockSpec((1, count, block), lambda s, c: (s, 0, c)),
            pl.BlockSpec((count // n, experts), lambda s, c: (s, 0)),
            pl.BlockSpec((experts, block), lambda s, c: (0, c)),
        ],
        out_specs=(
            pl.BlockSpec((held, 1, cap, block), lambda s, c: (0, s, 0, c)),
            pl.BlockSpec((count // n, block), lambda s, c: (s, c)),
        ),
    )(weights, gathered, logit, router_weight)


def local(n, m, tokens, grad_out, experts, gates, router_weight, saved_outputs):
    count, width = tokens.shape
    expert_count = router_weight.shape[0]
    layout = (expert_count // n, n, count // 2, width)
    info = jnp.concatenate(
        [experts.T.astype(F32), gates.T.astype(F32), jnp.zeros((4, count), F32)], axis=0
    )
    gathered, weights, logit, router_grad = exchange(
        info, grad_out, tokens, saved_outputs.reshape(layout), expert_count, n, m
    )
    expert_grad, input_grad = finish(weights, gathered, logit, router_weight, layout)
    return (input_grad, router_grad, expert_grad.reshape(saved_outputs.shape))


def solution(mesh):
    spec = P(("dp", "expert"), None)
    return jax.shard_map(
        functools.partial(local, mesh.shape["expert"], mesh.shape["dp"]),
        mesh=mesh,
        in_specs=(spec, spec, spec, spec, P(), spec),
        out_specs=(spec, P(), spec),
        check_vma=False,
    )
```

```python
import functools

import jax
import jax.numpy as jnp
from jax import lax
from jax.experimental import pallas as pl
from jax.experimental.pallas import tpu as pltpu
from jax.sharding import PartitionSpec as P

MESH = pl.DeviceIdType.MESH
F32 = jnp.float32
BF16 = jnp.bfloat16


def exchange_kernel(
    n, m, pieces, scale,
    experts_hbm, gates_hbm, g_hbm, tok_ref, rw_hbm, saved_ref,
    eg_hbm, ig_hbm, router_out,
    eg_out, ig_out, experts_v, gates_v, g_ref, rw_v, info_ref, weights_v, logit_v, slots, saved_v, tok_v, meta_own, meta_in, ret_own, ret_in,
    acc_a, acc_b, part, part_in, dp_in, fin, fin_in,
    g_send, g_recv, meta_send, meta_recv, ret_send, ret_recv,
    part_send, part_recv, dp_send, dp_recv, fin_send, fin_recv,
    saved_sem, load_sem, eg_sem, ig_sem,
):
    held, _, cap, width = saved_ref.shape
    rows = held * cap
    tokens = g_ref.shape[0]
    experts = rw_v.shape[0]
    piece = width // pieces
    share = width // n
    pairs = n // 2
    me = lax.axis_index("expert")
    dp = lax.axis_index("dp")
    parity = me % 2
    pair = me // 2

    def source(j):
        q, flip = j // 2, j % 2
        low = parity if flip == 0 else 1 - parity
        return ((pair - q + pairs) % pairs) * 2 + low

    def target(j):
        q, flip = j // 2, j % 2
        low = parity if flip == 0 else 1 - parity
        return ((pair + q) % pairs) * 2 + low

    def cols(c):
        return pl.ds(pl.multiple_of(c * piece, piece), piece)

    barrier = pltpu.get_barrier_semaphore()
    for j in range(1, n):
        pl.semaphore_signal(barrier, inc=1, device_id={"expert": target(j)}, device_id_type=MESH)

    def greet(i, carry):
        pl.semaphore_signal(barrier, inc=1, device_id={"dp": (dp + i) % m}, device_id_type=MESH)
        return carry

    lax.fori_loop(1, m, greet, 0)

    def saved_copy(j, h):
        return pltpu.make_async_copy(
            saved_ref.at[h, source(j)],
            saved_v.at[j, pl.ds(h * cap, cap)],
            saved_sem.at[j, h],
        )

    loads = [
        pltpu.make_async_copy(src, dst, load_sem.at[i])
        for i, (src, dst) in enumerate(
            [
                (experts_hbm, experts_v),
                (gates_hbm, gates_v),
                (g_hbm, g_ref),
                (tok_ref, tok_v),
                (rw_hbm, rw_v),
            ]
        )
    ]
    for copy in loads[:3]:
        copy.start()
    for j in range(n):
        for h in range(held):
            saved_copy(j, h).start()
    for copy in loads[3:]:
        copy.start()

    loads[0].wait()
    loads[1].wait()
    info_ref[...] = jnp.concatenate(
        [experts_v[...].astype(F32), gates_v[...].astype(F32), jnp.zeros((4, tokens), F32)], axis=0
    )

    expert_ids = lax.broadcasted_iota(jnp.int32, (experts, tokens), 0).astype(F32)
    hot = [(info_ref[k : k + 1, :] == expert_ids).astype(F32) for k in range(2)]
    earlier = (
        lax.broadcasted_iota(jnp.int32, (tokens, tokens), 0)
        < lax.broadcasted_iota(jnp.int32, (tokens, tokens), 1)
    ).astype(F32).astype(BF16)
    before = jnp.dot((hot[0] + hot[1]).astype(BF16), earlier, preferred_element_type=F32)
    meta_own[...] = info_ref[...]
    for k in range(2):
        position = jnp.sum(before * hot[k], axis=0, keepdims=True)
        meta_own[k : k + 1, :] = info_ref[k : k + 1, :] * float(cap) + position

    loads[2].wait()
    pl.semaphore_wait(barrier, n + m - 2)

    def g_copy(src, j, c, to):
        return pltpu.make_async_remote_copy(
            src_ref=src,
            dst_ref=slots.at[j - 1, :, cols(c)],
            send_sem=g_send.at[j - 1, c],
            recv_sem=g_recv.at[j - 1, c],
            device_id={"expert": to},
            device_id_type=MESH,
        )

    def small_copy(src, dst, send, recv, j, to):
        return pltpu.make_async_remote_copy(
            src_ref=src,
            dst_ref=dst.at[j - 1],
            send_sem=send.at[j - 1],
            recv_sem=recv.at[j - 1],
            device_id={"expert": to},
            device_id_type=MESH,
        )

    meta_copies = [
        small_copy(meta_own, meta_in, meta_send, meta_recv, j, target(j)) for j in range(1, n)
    ]
    for copy in meta_copies:
        copy.start()
    for q in range(1, pairs):

        def send_direct(c, carry, q=q):
            g_copy(g_ref.at[:, cols(c)], 2 * q, c, target(2 * q)).start()
            return carry

        lax.fori_loop(0, pieces, send_direct, 0)

    def send_partner(c, carry):
        g_copy(g_ref.at[:, cols(c)], 1, c, target(1)).start()
        return carry

    lax.fori_loop(0, pieces, send_partner, 0)

    row_ids = lax.broadcasted_iota(jnp.int32, (rows, tokens), 0).astype(F32)
    base = (me * rows).astype(F32)

    def masks(meta):
        return [meta[k : k + 1, :] - base == row_ids for k in range(2)]

    def write_weights(j, meta):
        named = masks(meta)
        weights = jnp.where(named[0], meta[2:3, :], 0.0) + jnp.where(named[1], meta[3:4, :], 0.0)
        weights_v[j] = weights.astype(BF16)

    def spread(j, c, right):
        block = jnp.dot(weights_v[j], right, preferred_element_type=F32).astype(BF16)
        for h in range(held):
            eg_out[h, source(j), :, cols(c)] = block[h * cap : (h + 1) * cap]

    def product(j, c, right):
        return lax.dot_general(
            saved_v[j, :, cols(c)], right, (((1,), (1,)), ((), ())), preferred_element_type=F32
        )

    def picked(meta, total):
        return [
            jnp.sum(jnp.where(named, total, 0.0), axis=0, keepdims=True) for named in masks(meta)
        ]

    def wait_saved(j):
        for h in range(held):
            saved_copy(j, h).wait()

    ret_copies = [
        small_copy(ret_own.at[j - 1], ret_in, ret_send, ret_recv, j, source(j))
        for j in range(1, n)
    ]

    def give_back(j, total):
        first, second = picked(meta_in[j - 1], total)
        ret_own[j - 1, 0:1, :] = first
        ret_own[j - 1, 1:2, :] = second
        ret_copies[j - 1].start()

    ret_own[...] = jnp.zeros_like(ret_own)
    wait_saved(0)
    write_weights(0, meta_own[...])
    zero = jnp.zeros((rows, tokens), F32)

    def own_step(c, total):
        spread(0, c, g_ref[:, cols(c)])
        return total + product(0, c, g_ref[:, cols(c)])

    own_total = lax.fori_loop(0, pieces, own_step, zero)
    store_copies = []

    def put_out(j):
        for h in range(held):
            copy = pltpu.make_async_copy(
                eg_out.at[h, source(j)], eg_hbm.at[h, source(j)], eg_sem.at[j, h]
            )
            copy.start()
            store_copies.append(copy)

    put_out(0)
    own_first, own_second = picked(meta_own[...], own_total)

    for j in range(1, n):
        meta_copies[j - 1].wait_recv()
        write_weights(j, meta_in[j - 1])

    def arrived(j, c):
        g_copy(slots.at[j - 1, :, cols(c)], j, c, target(j)).wait_recv()

    def take(j, c, acc):
        acc[...] += product(j, c, slots[j - 1, :, cols(c)])
        spread(j, c, slots[j - 1, :, cols(c)])

    acc_a[...] = zero
    wait_saved(1)

    def partner_step(c, carry):
        arrived(1, c)
        take(1, c, acc_a)
        return carry

    lax.fori_loop(0, pieces, partner_step, 0)
    give_back(1, acc_a[...])
    put_out(1)

    for q in range(1, pairs):
        direct, relayed = 2 * q, 2 * q + 1
        acc_a[...] = zero
        acc_b[...] = zero
        wait_saved(direct)
        wait_saved(relayed)

        def direct_step(c, direct=direct, relayed=relayed):
            arrived(direct, c)
            g_copy(slots.at[direct - 1, :, cols(c)], relayed, c, target(1)).start()
            take(direct, c, acc_a)

        def relayed_step(c, relayed=relayed):
            arrived(relayed, c)
            take(relayed, c, acc_b)

        direct_step(0)

        def step(c, carry, direct_step=direct_step, relayed_step=relayed_step):
            direct_step(c)
            relayed_step(c - 1)
            return carry

        lax.fori_loop(1, pieces, step, 0)
        give_back(direct, acc_a[...])
        relayed_step(pieces - 1)
        give_back(relayed, acc_b[...])
        put_out(direct)
        put_out(relayed)

    grads = [own_first, own_second]
    for j in range(1, n):
        ret_copies[j - 1].wait_recv()
        grads = [grads[k] + ret_in[j - 1, k : k + 1, :] for k in range(2)]
    gates = [info_ref[2 + k : 3 + k, :] for k in range(2)]
    blended = gates[0] * grads[0] + gates[1] * grads[1]
    logit = hot[0] * (gates[0] * (grads[0] - blended)) + hot[1] * (gates[1] * (grads[1] - blended))
    logit_low = logit.astype(BF16)
    loads[3].wait()
    for j in range(n):
        part[j] = jnp.dot(
            logit_low, tok_v[:, j * share : (j + 1) * share], preferred_element_type=F32
        )

    part_copies = [
        small_copy(part.at[target(j)], part_in, part_send, part_recv, j, target(j))
        for j in range(1, n)
    ]
    for copy in part_copies:
        copy.start()
    logit_v[...] = logit.T.astype(BF16)
    total = part[me]
    for j in range(1, n):
        part_copies[j - 1].wait_recv()
        total = total + part_in[j - 1]
    dp_in[dp] = total

    def dp_copy(slot, i):
        return pltpu.make_async_remote_copy(
            src_ref=dp_in.at[dp],
            dst_ref=dp_in.at[slot],
            send_sem=dp_send.at[i],
            recv_sem=dp_recv.at[i],
            device_id={"dp": (dp + i) % m},
            device_id_type=MESH,
        )

    def dp_start(i, carry):
        dp_copy(dp, i).start()
        return carry

    def dp_wait(i, carry):
        dp_copy((dp - i + m) % m, i).wait_recv()
        return carry

    lax.fori_loop(1, m, dp_start, 0)
    loads[4].wait()

    def input_step(c, carry):
        ig_out[:, cols(c)] = jnp.dot(
            logit_v[...], rw_v[:, cols(c)], preferred_element_type=F32
        ).astype(BF16)
        return carry

    lax.fori_loop(0, pieces, input_step, 0)
    ig_copy = pltpu.make_async_copy(ig_out, ig_hbm, ig_sem)
    ig_copy.start()
    store_copies.append(ig_copy)
    lax.fori_loop(1, m, dp_wait, 0)
    fin[...] = (
        lax.fori_loop(0, m, lambda i, t: t + dp_in[i], jnp.zeros((experts, share), F32)) * scale
    )
    fin_copies = [small_copy(fin, fin_in, fin_send, fin_recv, j, target(j)) for j in range(1, n)]
    for copy in fin_copies:
        copy.start()

    def lanes(k):
        return pl.ds(pl.multiple_of(k * share, share), share)

    router_out[:, lanes(me)] = fin[...]

    def g_sent(c, carry):
        g_copy(g_ref.at[:, cols(c)], 1, c, target(1)).wait_send()
        for q in range(1, pairs):
            g_copy(g_ref.at[:, cols(c)], 2 * q, c, target(2 * q)).wait_send()
            g_copy(slots.at[2 * q - 1, :, cols(c)], 2 * q + 1, c, target(1)).wait_send()
        return carry

    lax.fori_loop(0, pieces, g_sent, 0)

    def dp_sent(i, carry):
        dp_copy(dp, i).wait_send()
        return carry

    lax.fori_loop(1, m, dp_sent, 0)
    for copy in meta_copies + ret_copies + part_copies + fin_copies:
        copy.wait_send()
    for copy in store_copies:
        copy.wait()
    for j in range(1, n):
        fin_copies[j - 1].wait_recv()
        router_out[:, lanes(source(j))] = fin_in[j - 1]


def exchange(experts, gates, grad_out, tokens, router_weight, saved, n, m):
    held, _, cap, width = saved.shape
    count = tokens.shape[0]
    expert_count = router_weight.shape[0]
    rows = held * cap
    pieces = max(1, width // 512)
    share = width // n
    scale = float(m * n * count) ** (-0.5)
    dma = pltpu.SemaphoreType.DMA
    vmem = pl.BlockSpec(memory_space=pltpu.VMEM)
    hbm = pl.BlockSpec(memory_space=pltpu.HBM)
    return pl.pallas_call(
        functools.partial(exchange_kernel, n, m, pieces, scale),
        name="exchange",
        out_shape=(
            jax.ShapeDtypeStruct((held, n, cap, width), BF16),
            jax.ShapeDtypeStruct((count, width), BF16),
            jax.ShapeDtypeStruct((expert_count, width), F32),
        ),
        in_specs=[hbm] * 6,
        out_specs=(hbm, hbm, vmem),
        scratch_shapes=[
            pltpu.VMEM((held, n, cap, width), BF16),
            pltpu.VMEM((count, width), BF16),
            pltpu.VMEM(experts.shape, experts.dtype),
            pltpu.VMEM(gates.shape, gates.dtype),
            pltpu.VMEM((count, width), BF16),
            pltpu.VMEM((expert_count, width), BF16),
            pltpu.VMEM((8, count), F32),
            pltpu.VMEM((n, rows, count), BF16),
            pltpu.VMEM((count, expert_count), BF16),
            pltpu.VMEM((n - 1, count, width), BF16),
            pltpu.VMEM((n, rows, width), BF16),
            pltpu.VMEM((count, width), BF16),
            pltpu.VMEM((8, count), F32),
            pltpu.VMEM((n - 1, 8, count), F32),
            pltpu.VMEM((n - 1, 8, count), F32),
            pltpu.VMEM((n - 1, 8, count), F32),
            pltpu.VMEM((rows, count), F32),
            pltpu.VMEM((rows, count), F32),
            pltpu.VMEM((n, expert_count, share), F32),
            pltpu.VMEM((n - 1, expert_count, share), F32),
            pltpu.VMEM((m, expert_count, share), F32),
            pltpu.VMEM((expert_count, share), F32),
            pltpu.VMEM((n - 1, expert_count, share), F32),
            dma((n - 1, pieces)), dma((n - 1, pieces)),
            dma((n - 1,)), dma((n - 1,)),
            dma((n - 1,)), dma((n - 1,)),
            dma((n - 1,)), dma((n - 1,)),
            dma((m,)), dma((m,)),
            dma((n - 1,)), dma((n - 1,)),
            dma((n, held)), dma((5,)), dma((n, held)), dma,
        ],
        compiler_params=pltpu.CompilerParams(
            collective_id=0, has_side_effects=True, vmem_limit_bytes=58 << 20
        ),
    )(experts, gates, grad_out, tokens, router_weight, saved)


def store_kernel(
    eg_ref, ig_ref, router_ref, eg_out, ig_out, router_out, eg_v, ig_v, router_v, in_sem, out_sem
):
    held, n = eg_ref.shape[:2]
    steps = [
        (src.at[h, s], buf.at[h, s], dst.at[h, s])
        for src, buf, dst in [(eg_ref, eg_v, eg_out)]
        for h in range(held)
        for s in range(n)
    ]
    half = ig_ref.shape[0] // 2
    for k in range(2):
        part = pl.ds(k * half, half)
        steps.append((ig_ref.at[part], ig_v.at[part], ig_out.at[part]))
    steps.append((router_ref, router_v, router_out))
    loads = [
        pltpu.make_async_copy(src, buf, in_sem.at[i]) for i, (src, buf, _) in enumerate(steps)
    ]
    stores = [
        pltpu.make_async_copy(buf, dst, out_sem.at[i]) for i, (_, buf, dst) in enumerate(steps)
    ]
    for copy in loads:
        copy.start()
    for load, put in zip(loads, stores):
        load.wait()
        put.start()
    for copy in stores:
        copy.wait()


def store(expert_grad, input_grad, router_grad):
    held, n = expert_grad.shape[:2]
    hbm = pl.BlockSpec(memory_space=pltpu.HBM)
    arrays = (expert_grad, input_grad, router_grad)
    count = held * n + 3
    return pl.pallas_call(
        store_kernel,
        name="finish",
        out_shape=tuple(jax.ShapeDtypeStruct(a.shape, a.dtype) for a in arrays),
        in_specs=[hbm] * 3,
        out_specs=(hbm,) * 3,
        scratch_shapes=[
            *[pltpu.VMEM(a.shape, a.dtype) for a in arrays],
            pltpu.SemaphoreType.DMA((count,)),
            pltpu.SemaphoreType.DMA((count,)),
        ],
        compiler_params=pltpu.CompilerParams(vmem_limit_bytes=58 << 20),
    )(*arrays)


def local(n, m, tokens, grad_out, experts, gates, router_weight, saved_outputs):
    count, width = tokens.shape
    layout = (router_weight.shape[0] // n, n, count // 2, width)
    results = exchange(
        experts.T, gates.T, grad_out, tokens, router_weight, saved_outputs.reshape(layout), n, m
    )
    expert_grad, input_grad, router_grad = store(*results)
    return (input_grad, router_grad, expert_grad.reshape(saved_outputs.shape))


def solution(mesh):
    spec = P(("dp", "expert"), None)
    return jax.shard_map(
        functools.partial(local, mesh.shape["expert"], mesh.shape["dp"]),
        mesh=mesh,
        in_specs=(spec, spec, spec, spec, P(), spec),
        out_specs=(spec, P(), spec),
        check_vma=False,
    )
```

```python
import functools

import jax
import jax.numpy as jnp
from jax import lax
from jax.experimental import pallas as pl
from jax.experimental.pallas import tpu as pltpu
from jax.sharding import PartitionSpec as P

MESH = pl.DeviceIdType.MESH
F32 = jnp.float32
BF16 = jnp.bfloat16


def exchange_kernel(
    n, m, pieces, scale,
    experts_hbm, gates_hbm, g_hbm, tok_ref, rw_hbm, saved_ref,
    eg_hbm, ig_hbm, router_out,
    eg_out, ig_out, experts_v, gates_v, g_ref, rw_v, info_ref, weights_v, logit_v, slots, saved_v, tok_v, meta_own, meta_in, ret_own, ret_in,
    acc_a, acc_b, part, part_in, dp_in, fin, fin_in,
    g_send, g_recv, meta_send, meta_recv, ret_send, ret_recv,
    part_send, part_recv, dp_send, dp_recv, fin_send, fin_recv,
    saved_sem, load_sem, eg_sem, ig_sem,
):
    held, _, cap, width = saved_ref.shape
    rows = held * cap
    tokens = g_ref.shape[0]
    experts = rw_v.shape[0]
    piece = width // pieces
    share = width // n
    pairs = n // 2
    me = lax.axis_index("expert")
    dp = lax.axis_index("dp")
    parity = me % 2
    pair = me // 2

    def source(j):
        q, flip = j // 2, j % 2
        low = parity if flip == 0 else 1 - parity
        return ((pair - q + pairs) % pairs) * 2 + low

    def target(j):
        q, flip = j // 2, j % 2
        low = parity if flip == 0 else 1 - parity
        return ((pair + q) % pairs) * 2 + low

    def cols(c):
        return pl.ds(pl.multiple_of(c * piece, piece), piece)

    barrier = pltpu.get_barrier_semaphore()
    for j in range(1, n):
        pl.semaphore_signal(barrier, inc=1, device_id={"expert": target(j)}, device_id_type=MESH)

    def greet(i, carry):
        pl.semaphore_signal(barrier, inc=1, device_id={"dp": (dp + i) % m}, device_id_type=MESH)
        return carry

    lax.fori_loop(1, m, greet, 0)

    def saved_copy(j, h):
        return pltpu.make_async_copy(
            saved_ref.at[h, source(j)],
            saved_v.at[j, pl.ds(h * cap, cap)],
            saved_sem.at[j, h],
        )

    loads = [
        pltpu.make_async_copy(src, dst, load_sem.at[i])
        for i, (src, dst) in enumerate(
            [
                (experts_hbm, experts_v),
                (gates_hbm, gates_v),
                (g_hbm, g_ref),
                (tok_ref, tok_v),
                (rw_hbm, rw_v),
            ]
        )
    ]
    for copy in loads[:3]:
        copy.start()
    for j in range(n):
        for h in range(held):
            saved_copy(j, h).start()
    for copy in loads[3:]:
        copy.start()

    loads[0].wait()
    loads[1].wait()
    info_ref[...] = jnp.concatenate(
        [experts_v[...].astype(F32), gates_v[...].astype(F32), jnp.zeros((4, tokens), F32)], axis=0
    )

    expert_ids = lax.broadcasted_iota(jnp.int32, (experts, tokens), 0).astype(F32)
    hot = [(info_ref[k : k + 1, :] == expert_ids).astype(F32) for k in range(2)]
    earlier = (
        lax.broadcasted_iota(jnp.int32, (tokens, tokens), 0)
        < lax.broadcasted_iota(jnp.int32, (tokens, tokens), 1)
    ).astype(F32).astype(BF16)
    before = jnp.dot((hot[0] + hot[1]).astype(BF16), earlier, preferred_element_type=F32)
    meta_own[...] = info_ref[...]
    for k in range(2):
        position = jnp.sum(before * hot[k], axis=0, keepdims=True)
        meta_own[k : k + 1, :] = info_ref[k : k + 1, :] * float(cap) + position

    loads[2].wait()
    pl.semaphore_wait(barrier, n + m - 2)

    def g_copy(src, j, c, to):
        return pltpu.make_async_remote_copy(
            src_ref=src,
            dst_ref=slots.at[j - 1, :, cols(c)],
            send_sem=g_send.at[j - 1, c],
            recv_sem=g_recv.at[j - 1, c],
            device_id={"expert": to},
            device_id_type=MESH,
        )

    def small_copy(src, dst, send, recv, j, to):
        return pltpu.make_async_remote_copy(
            src_ref=src,
            dst_ref=dst.at[j - 1],
            send_sem=send.at[j - 1],
            recv_sem=recv.at[j - 1],
            device_id={"expert": to},
            device_id_type=MESH,
        )

    meta_copies = [
        small_copy(meta_own, meta_in, meta_send, meta_recv, j, target(j)) for j in range(1, n)
    ]
    for copy in meta_copies:
        copy.start()
    for q in range(1, pairs):

        def send_direct(c, carry, q=q):
            g_copy(g_ref.at[:, cols(c)], 2 * q, c, target(2 * q)).start()
            return carry

        lax.fori_loop(0, pieces, send_direct, 0)

    def send_partner(c, carry):
        g_copy(g_ref.at[:, cols(c)], 1, c, target(1)).start()
        return carry

    lax.fori_loop(0, pieces, send_partner, 0)

    row_ids = lax.broadcasted_iota(jnp.int32, (rows, tokens), 0).astype(F32)
    base = (me * rows).astype(F32)

    def masks(meta):
        return [meta[k : k + 1, :] - base == row_ids for k in range(2)]

    def write_weights(j, meta):
        named = masks(meta)
        weights = jnp.where(named[0], meta[2:3, :], 0.0) + jnp.where(named[1], meta[3:4, :], 0.0)
        weights_v[j] = weights.astype(BF16)

    def spread(j, c, right):
        block = jnp.dot(weights_v[j], right, preferred_element_type=F32).astype(BF16)
        for h in range(held):
            eg_out[h, source(j), :, cols(c)] = block[h * cap : (h + 1) * cap]

    def product(j, c, right):
        return lax.dot_general(
            saved_v[j, :, cols(c)], right, (((1,), (1,)), ((), ())), preferred_element_type=F32
        )

    def picked(meta, total):
        return [
            jnp.sum(jnp.where(named, total, 0.0), axis=0, keepdims=True) for named in masks(meta)
        ]

    def wait_saved(j):
        for h in range(held):
            saved_copy(j, h).wait()

    ret_copies = [
        small_copy(ret_own.at[j - 1], ret_in, ret_send, ret_recv, j, source(j))
        for j in range(1, n)
    ]

    def give_back(j, total):
        first, second = picked(meta_in[j - 1], total)
        ret_own[j - 1, 0:1, :] = first
        ret_own[j - 1, 1:2, :] = second
        ret_copies[j - 1].start()

    ret_own[...] = jnp.zeros_like(ret_own)
    wait_saved(0)
    write_weights(0, meta_own[...])
    zero = jnp.zeros((rows, tokens), F32)

    def own_step(c, total):
        spread(0, c, g_ref[:, cols(c)])
        return total + product(0, c, g_ref[:, cols(c)])

    own_total = lax.fori_loop(0, pieces, own_step, zero)
    store_copies = []

    def put_out(j):
        for h in range(held):
            copy = pltpu.make_async_copy(
                eg_out.at[h, source(j)], eg_hbm.at[h, source(j)], eg_sem.at[j, h]
            )
            copy.start()
            store_copies.append(copy)

    put_out(0)
    own_first, own_second = picked(meta_own[...], own_total)

    for j in range(1, n):
        meta_copies[j - 1].wait_recv()
        write_weights(j, meta_in[j - 1])

    def arrived(j, c):
        g_copy(slots.at[j - 1, :, cols(c)], j, c, target(j)).wait_recv()

    def take(j, c, acc):
        acc[...] += product(j, c, slots[j - 1, :, cols(c)])
        spread(j, c, slots[j - 1, :, cols(c)])

    acc_a[...] = zero
    wait_saved(1)

    def partner_step(c, carry):
        arrived(1, c)
        take(1, c, acc_a)
        return carry

    lax.fori_loop(0, pieces, partner_step, 0)
    give_back(1, acc_a[...])
    put_out(1)

    for q in range(1, pairs):
        direct, relayed = 2 * q, 2 * q + 1
        acc_a[...] = zero
        acc_b[...] = zero
        wait_saved(direct)
        wait_saved(relayed)

        def direct_step(c, direct=direct, relayed=relayed):
            arrived(direct, c)
            g_copy(slots.at[direct - 1, :, cols(c)], relayed, c, target(1)).start()
            take(direct, c, acc_a)

        def relayed_step(c, relayed=relayed):
            arrived(relayed, c)
            take(relayed, c, acc_b)

        direct_step(0)

        def step(c, carry, direct_step=direct_step, relayed_step=relayed_step):
            direct_step(c)
            relayed_step(c - 1)
            return carry

        lax.fori_loop(1, pieces, step, 0)
        give_back(direct, acc_a[...])
        relayed_step(pieces - 1)
        give_back(relayed, acc_b[...])
        put_out(direct)
        put_out(relayed)

    grads = [own_first, own_second]
    for j in range(1, n):
        ret_copies[j - 1].wait_recv()
        grads = [grads[k] + ret_in[j - 1, k : k + 1, :] for k in range(2)]
    gates = [info_ref[2 + k : 3 + k, :] for k in range(2)]
    blended = gates[0] * grads[0] + gates[1] * grads[1]
    logit = hot[0] * (gates[0] * (grads[0] - blended)) + hot[1] * (gates[1] * (grads[1] - blended))
    logit_low = logit.astype(BF16)
    loads[3].wait()
    for j in range(n):
        part[j] = jnp.dot(
            logit_low, tok_v[:, j * share : (j + 1) * share], preferred_element_type=F32
        )

    part_copies = [
        small_copy(part.at[target(j)], part_in, part_send, part_recv, j, target(j))
        for j in range(1, n)
    ]
    for copy in part_copies:
        copy.start()
    logit_v[...] = logit.T.astype(BF16)
    total = part[me]
    for j in range(1, n):
        part_copies[j - 1].wait_recv()
        total = total + part_in[j - 1]
    dp_in[dp] = total.astype(BF16)

    def dp_copy(slot, i):
        return pltpu.make_async_remote_copy(
            src_ref=dp_in.at[dp],
            dst_ref=dp_in.at[slot],
            send_sem=dp_send.at[i],
            recv_sem=dp_recv.at[i],
            device_id={"dp": (dp + i) % m},
            device_id_type=MESH,
        )

    def dp_start(i, carry):
        dp_copy(dp, i).start()
        return carry

    def dp_wait(i, carry):
        dp_copy((dp - i + m) % m, i).wait_recv()
        return carry

    lax.fori_loop(1, m, dp_start, 0)
    loads[4].wait()

    def input_step(c, carry):
        ig_out[:, cols(c)] = jnp.dot(
            logit_v[...], rw_v[:, cols(c)], preferred_element_type=F32
        ).astype(BF16)
        return carry

    lax.fori_loop(0, pieces, input_step, 0)
    ig_copy = pltpu.make_async_copy(ig_out, ig_hbm, ig_sem)
    ig_copy.start()
    store_copies.append(ig_copy)
    lax.fori_loop(1, m, dp_wait, 0)
    fin[...] = (
        lax.fori_loop(0, m, lambda i, t: t + dp_in[i].astype(F32), jnp.zeros((experts, share), F32)) * scale
    )
    fin_copies = [small_copy(fin, fin_in, fin_send, fin_recv, j, target(j)) for j in range(1, n)]
    for copy in fin_copies:
        copy.start()

    def lanes(k):
        return pl.ds(pl.multiple_of(k * share, share), share)

    router_out[:, lanes(me)] = fin[...]

    def g_sent(c, carry):
        g_copy(g_ref.at[:, cols(c)], 1, c, target(1)).wait_send()
        for q in range(1, pairs):
            g_copy(g_ref.at[:, cols(c)], 2 * q, c, target(2 * q)).wait_send()
            g_copy(slots.at[2 * q - 1, :, cols(c)], 2 * q + 1, c, target(1)).wait_send()
        return carry

    lax.fori_loop(0, pieces, g_sent, 0)

    def dp_sent(i, carry):
        dp_copy(dp, i).wait_send()
        return carry

    lax.fori_loop(1, m, dp_sent, 0)
    for copy in meta_copies + ret_copies + part_copies + fin_copies:
        copy.wait_send()
    for copy in store_copies:
        copy.wait()
    for j in range(1, n):
        fin_copies[j - 1].wait_recv()
        router_out[:, lanes(source(j))] = fin_in[j - 1]


def exchange(experts, gates, grad_out, tokens, router_weight, saved, n, m):
    held, _, cap, width = saved.shape
    count = tokens.shape[0]
    expert_count = router_weight.shape[0]
    rows = held * cap
    pieces = max(1, width // 512)
    share = width // n
    scale = float(m * n * count) ** (-0.5)
    dma = pltpu.SemaphoreType.DMA
    vmem = pl.BlockSpec(memory_space=pltpu.VMEM)
    hbm = pl.BlockSpec(memory_space=pltpu.HBM)
    return pl.pallas_call(
        functools.partial(exchange_kernel, n, m, pieces, scale),
        name="exchange",
        out_shape=(
            jax.ShapeDtypeStruct((held, n, cap, width), BF16),
            jax.ShapeDtypeStruct((count, width), BF16),
            jax.ShapeDtypeStruct((expert_count, width), F32),
        ),
        in_specs=[hbm] * 6,
        out_specs=(hbm, hbm, vmem),
        scratch_shapes=[
            pltpu.VMEM((held, n, cap, width), BF16),
            pltpu.VMEM((count, width), BF16),
            pltpu.VMEM(experts.shape, experts.dtype),
            pltpu.VMEM(gates.shape, gates.dtype),
            pltpu.VMEM((count, width), BF16),
            pltpu.VMEM((expert_count, width), BF16),
            pltpu.VMEM((8, count), F32),
            pltpu.VMEM((n, rows, count), BF16),
            pltpu.VMEM((count, expert_count), BF16),
            pltpu.VMEM((n - 1, count, width), BF16),
            pltpu.VMEM((n, rows, width), BF16),
            pltpu.VMEM((count, width), BF16),
            pltpu.VMEM((8, count), F32),
            pltpu.VMEM((n - 1, 8, count), F32),
            pltpu.VMEM((n - 1, 8, count), F32),
            pltpu.VMEM((n - 1, 8, count), F32),
            pltpu.VMEM((rows, count), F32),
            pltpu.VMEM((rows, count), F32),
            pltpu.VMEM((n, expert_count, share), F32),
            pltpu.VMEM((n - 1, expert_count, share), F32),
            pltpu.VMEM((m, expert_count, share), BF16),
            pltpu.VMEM((expert_count, share), F32),
            pltpu.VMEM((n - 1, expert_count, share), F32),
            dma((n - 1, pieces)), dma((n - 1, pieces)),
            dma((n - 1,)), dma((n - 1,)),
            dma((n - 1,)), dma((n - 1,)),
            dma((n - 1,)), dma((n - 1,)),
            dma((m,)), dma((m,)),
            dma((n - 1,)), dma((n - 1,)),
            dma((n, held)), dma((5,)), dma((n, held)), dma,
        ],
        compiler_params=pltpu.CompilerParams(
            collective_id=0, has_side_effects=True, vmem_limit_bytes=58 << 20
        ),
    )(experts, gates, grad_out, tokens, router_weight, saved)


def store_kernel(
    eg_ref, ig_ref, router_ref, eg_out, ig_out, router_out, eg_v, ig_v, router_v, in_sem, out_sem
):
    held, n = eg_ref.shape[:2]
    steps = [
        (src.at[h, s], buf.at[h, s], dst.at[h, s])
        for src, buf, dst in [(eg_ref, eg_v, eg_out)]
        for h in range(held)
        for s in range(n)
    ]
    half = ig_ref.shape[0] // 2
    for k in range(2):
        part = pl.ds(k * half, half)
        steps.append((ig_ref.at[part], ig_v.at[part], ig_out.at[part]))
    steps.append((router_ref, router_v, router_out))
    loads = [
        pltpu.make_async_copy(src, buf, in_sem.at[i]) for i, (src, buf, _) in enumerate(steps)
    ]
    stores = [
        pltpu.make_async_copy(buf, dst, out_sem.at[i]) for i, (_, buf, dst) in enumerate(steps)
    ]
    for copy in loads:
        copy.start()
    for load, put in zip(loads, stores):
        load.wait()
        put.start()
    for copy in stores:
        copy.wait()


def store(expert_grad, input_grad, router_grad):
    held, n = expert_grad.shape[:2]
    hbm = pl.BlockSpec(memory_space=pltpu.HBM)
    arrays = (expert_grad, input_grad, router_grad)
    count = held * n + 3
    return pl.pallas_call(
        store_kernel,
        name="finish",
        out_shape=tuple(jax.ShapeDtypeStruct(a.shape, a.dtype) for a in arrays),
        in_specs=[hbm] * 3,
        out_specs=(hbm,) * 3,
        scratch_shapes=[
            *[pltpu.VMEM(a.shape, a.dtype) for a in arrays],
            pltpu.SemaphoreType.DMA((count,)),
            pltpu.SemaphoreType.DMA((count,)),
        ],
        compiler_params=pltpu.CompilerParams(vmem_limit_bytes=58 << 20),
    )(*arrays)


def local(n, m, tokens, grad_out, experts, gates, router_weight, saved_outputs):
    count, width = tokens.shape
    layout = (router_weight.shape[0] // n, n, count // 2, width)
    results = exchange(
        experts.T, gates.T, grad_out, tokens, router_weight, saved_outputs.reshape(layout), n, m
    )
    expert_grad, input_grad, router_grad = store(*results)
    return (input_grad, router_grad, expert_grad.reshape(saved_outputs.shape))


def solution(mesh):
    spec = P(("dp", "expert"), None)
    return jax.shard_map(
        functools.partial(local, mesh.shape["expert"], mesh.shape["dp"]),
        mesh=mesh,
        in_specs=(spec, spec, spec, spec, P(), spec),
        out_specs=(spec, P(), spec),
        check_vma=False,
    )
```
